32 devices in a mesh: dp: 8 (over z, y), cp: 4 (over x, core).
Axes of the slice: x: 2, y: 2, z: 4, core: 2. Of those that a mesh axis runs over, the one named last changes fastest.
Arguments:
- hidden: bfloat16 [128, 1024, 2048], P('dp', 'cp')
- positions: int32 [1024], P('cp')
- w_q: bfloat16 [2048, 2048], replicated
- w_k: bfloat16 [2048, 2048], replicated
- w_v: bfloat16 [2048, 2048], replicated
- w_o: bfloat16 [2048, 2048], replicated
Outputs:
- output 1: bfloat16 [128, 1024, 2048], P('dp', 'cp')
- output 2: float32 [16], replicated
- output 3: bfloat16 [2048, 2048], replicated
- output 4: bfloat16 [2048, 2048], replicated
All inputs are finite; a program needn't handle non-finite values.
Results may differ from the reference program's by a relative error of at most 0.00757875.
Values are sent between devices in bfloat16 or wider.
A program may use at most 1 GiB of HBM per device.

```python
import jax
import jax.numpy as jnp
from jax import lax

BATCH_SIZE = 128
SEQ_LEN = 1024
D_MODEL = 2048
NUM_HEADS = 16
QUERY_BLOCK = 64
HEAD_DIM = 128
TAU_CLIP = 100
ROPE_THETA = 50000


def rope_rotate(tensor, pos_ids):
    half_dim = HEAD_DIM // 2
    inv_freq = jnp.float32(ROPE_THETA) ** (-jnp.arange(half_dim, dtype=jnp.float32) * (2.0 / HEAD_DIM))
    angle = pos_ids.astype(jnp.float32)[:, None] * inv_freq[None, :]
    cos_t = jnp.cos(angle)[:, None, :]
    sin_t = jnp.sin(angle)[:, None, :]
    lead_half = tensor[..., :half_dim]
    tail_half = tensor[..., half_dim:]
    return jnp.concatenate([lead_half * cos_t - tail_half * sin_t, tail_half * cos_t + lead_half * sin_t], axis=-1)


def setup_inputs(seed: int = 0) -> dict:
    root_key = jax.random.key(seed)
    sub_keys = jax.random.split(root_key, 15)
    width = NUM_HEADS * HEAD_DIM
    gaps = jax.random.randint(sub_keys[0], (SEQ_LEN,), 1, 3)
    start_pos = jax.random.randint(sub_keys[1], (), 0, SEQ_LEN // 2 + 1)
    positions = (start_pos + jnp.cumsum(gaps) - 1).astype(jnp.int32)
    spike_row = jax.random.randint(sub_keys[2], (), 0, BATCH_SIZE)
    key_slot = jax.random.randint(sub_keys[3], (), 0, SEQ_LEN // 2)
    query_slot = jax.random.randint(sub_keys[4], (), SEQ_LEN // 2, SEQ_LEN)
    clip_heads = (jax.random.permutation(sub_keys[5], NUM_HEADS) < NUM_HEADS // 2).astype(jnp.float32)
    head_gain = jax.random.uniform(sub_keys[6], (NUM_HEADS,), jnp.float32, 1.0, 1.25)
    dir_query = jax.random.normal(sub_keys[7], (D_MODEL,), jnp.float32)
    dir_query = dir_query / jnp.sqrt(jnp.sum(dir_query * dir_query))
    dir_key = jax.random.normal(sub_keys[8], (D_MODEL,), jnp.float32)
    dir_key = dir_key / jnp.sqrt(jnp.sum(dir_key * dir_key))
    plant_q = jax.random.normal(sub_keys[9], (NUM_HEADS, HEAD_DIM), jnp.float32)
    plant_q = plant_q / jnp.sqrt(jnp.mean(plant_q * plant_q, axis=-1, keepdims=True))
    plant_q = plant_q * (4.0 * head_gain * clip_heads)[:, None] * D_MODEL ** -0.5
    delta = positions[query_slot] - positions[key_slot]
    plant_k = rope_rotate(plant_q[None], delta[None])[0]
    noise_scale = 1.5 * D_MODEL ** -0.5
    w_q = noise_scale * jax.random.normal(sub_keys[10], (D_MODEL, width), jnp.float32) + dir_query[:, None] * plant_q.reshape(width)[None, :]
    w_k = noise_scale * jax.random.normal(sub_keys[11], (D_MODEL, width), jnp.float32) + dir_key[:, None] * plant_k.reshape(width)[None, :]
    w_v = jax.random.normal(sub_keys[12], (D_MODEL, width), jnp.float32) * D_MODEL ** -0.5
    w_o = jax.random.normal(sub_keys[13], (width, D_MODEL), jnp.float32) * width ** -0.5
    hidden = jax.random.normal(sub_keys[14], (BATCH_SIZE, SEQ_LEN, D_MODEL), jnp.float32)
    spike_scale = jnp.sqrt(jnp.float32(D_MODEL))
    hidden = hidden.at[spike_row, query_slot].set(spike_scale * dir_query)
    hidden = hidden.at[spike_row, key_slot].set(spike_scale * dir_key)
    return {
        "hidden": hidden.astype(jnp.bfloat16),
        "positions": positions,
        "w_q": w_q.astype(jnp.bfloat16),
        "w_k": w_k.astype(jnp.bfloat16),
        "w_v": w_v.astype(jnp.bfloat16),
        "w_o": w_o.astype(jnp.bfloat16),
    }


def reference(hidden, positions, w_q, w_k, w_v, w_o):
    score_scale = HEAD_DIM ** -0.5
    n_blocks = SEQ_LEN // QUERY_BLOCK
    pos_blocks = positions.reshape(n_blocks, QUERY_BLOCK)
    head_shape = (SEQ_LEN, NUM_HEADS, HEAD_DIM)

    def one_row(row_in):
        q_all = rope_rotate(jnp.dot(row_in, w_q, preferred_element_type=jnp.float32).reshape(head_shape), positions).astype(jnp.bfloat16)
        k_all = rope_rotate(jnp.dot(row_in, w_k, preferred_element_type=jnp.float32).reshape(head_shape), positions).astype(jnp.bfloat16)
        v_all = jnp.dot(row_in, w_v, preferred_element_type=jnp.float32).astype(jnp.bfloat16).reshape(head_shape)
        k_wide = k_all.astype(jnp.float32)
        v_wide = v_all.astype(jnp.float32)
        q_blocks = q_all.reshape(n_blocks, QUERY_BLOCK, NUM_HEADS, HEAD_DIM)

        def one_block(block_in):
            q_blk, pos_blk = block_in
            scores = jnp.einsum("qhd,khd->hqk", q_blk.astype(jnp.float32), k_wide) * score_scale
            allowed = positions[None, None, :] <= pos_blk[None, :, None]
            scores = jnp.where(allowed, scores, -jnp.inf)
            block_max = jnp.max(scores, axis=(1, 2))
            prob_w = jax.nn.softmax(scores, axis=-1)
            attn_blk = jnp.einsum("hqk,khd->qhd", prob_w, v_wide)
            return attn_blk.astype(jnp.bfloat16), block_max

        attn_blocks, block_maxes = lax.map(one_block, (q_blocks, pos_blocks))
        attn_flat = attn_blocks.reshape(SEQ_LEN, NUM_HEADS * HEAD_DIM)
        row_out = jnp.dot(attn_flat, w_o, preferred_element_type=jnp.float32).astype(jnp.bfloat16)
        return row_out, jnp.max(block_maxes, axis=0)

    attn_out, row_maxes = lax.map(one_row, hidden)
    head_max = jnp.max(row_maxes, axis=0)
    factor = jnp.where(head_max > TAU_CLIP, jnp.sqrt(TAU_CLIP / head_max), 1.0)
    col_factor = jnp.repeat(factor, HEAD_DIM)
    w_q_new = (w_q.astype(jnp.float32) * col_factor[None, :]).astype(jnp.bfloat16)
    w_k_new = (w_k.astype(jnp.float32) * col_factor[None, :]).astype(jnp.bfloat16)
    return attn_out, head_max, w_q_new, w_k_new
```

```python
import functools

import jax
import jax.numpy as jnp
from jax import lax
from jax.experimental import pallas as pl
from jax.experimental.pallas import tpu as pltpu
from jax.sharding import PartitionSpec as P


HEAD_DIM = 128
TAU_CLIP = 100.0
ROPE_THETA = 50000.0
GROUP = 2 * HEAD_DIM
STEP_ROWS = 2
NEG = -1e30


def rope_tables(pos_ids):
    half_dim = HEAD_DIM // 2
    inv_freq = jnp.float32(ROPE_THETA) ** (-jnp.arange(half_dim, dtype=jnp.float32) * (2.0 / HEAD_DIM))
    angle = pos_ids.astype(jnp.float32)[:, None] * inv_freq[None, :]
    cos_t, sin_t = jnp.cos(angle), jnp.sin(angle)
    return jnp.concatenate([cos_t, cos_t], axis=-1), jnp.concatenate([-sin_t, sin_t], axis=-1)


def rows_kernel(whole, chained, piece, meta, x_own, x_sib, x_str, x_crs, w_q, w_k, w_v, w_o, cos_t, sin_t, *refs):
    if chained:
        refs = refs[1:]
    if whole:
        o_keep, o_send, o_str, o_crs, top, q_scr, k_scr, v_scr, att, wo_scr, sem = refs
    else:
        o_keep, o_send, top, q_scr, k_scr, v_scr, att, wo_scr, sem = refs
    step = pl.program_id(0)
    n_steps = pl.num_programs(0)
    chip, core = meta[0], meta[1]
    rows = STEP_ROWS
    local_off = 0 if whole else 2 * piece
    remote_off = 2 * piece if whole else 0
    scale = HEAD_DIM ** -0.5

    def wo_copy():
        return pltpu.make_async_copy(w_o, wo_scr, sem)

    def project(x_ref, slot, base, piece_id, with_q):
        x2 = x_ref[...].reshape(rows * piece, x_ref.shape[2])
        at = pl.multiple_of(base + slot * piece, piece)
        pos = pl.ds(pl.multiple_of(piece_id * piece, piece), piece)
        cos_p, sin_p = cos_t[pos, :], sin_t[pos, :]

        def rotated(w_ref, dst):
            t = jnp.dot(x2, w_ref[...], preferred_element_type=jnp.float32)
            for r in range(rows):
                for h in range(2):
                    th = t[r * piece:(r + 1) * piece, h * HEAD_DIM:(h + 1) * HEAD_DIM]
                    th = th * cos_p + pltpu.roll(th, HEAD_DIM // 2, axis=1) * sin_p
                    dst[r, pl.ds(at, piece), h * HEAD_DIM:(h + 1) * HEAD_DIM] = th.astype(jnp.bfloat16)

        if with_q:
            rotated(w_q, q_scr)
        rotated(w_k, k_scr)
        v = jnp.dot(x2, w_v[...], preferred_element_type=jnp.float32).astype(jnp.bfloat16)
        for r in range(rows):
            v_scr[r, pl.ds(at, piece), :] = v[r * piece:(r + 1) * piece]

    def attend(q_blocks, key_start, att_base):
        causal = lax.broadcasted_iota(jnp.int32, (piece, piece), 0) >= lax.broadcasted_iota(jnp.int32, (piece, piece), 1)
        nt = (((1,), (1,)), ((), ()))
        for h in range(2):
            cols = slice(h * HEAD_DIM, (h + 1) * HEAD_DIM)
            best = None
            for r in range(rows):
                for q_at in q_blocks:
                    q = q_scr[r, q_at:q_at + piece, cols]
                    s_diag = lax.dot_general(q, k_scr[r, q_at:q_at + piece, cols], nt, preferred_element_type=jnp.float32)
                    s_diag = jnp.where(causal, s_diag, NEG)
                    m = jnp.max(s_diag, axis=1, keepdims=True)
                    if q_at > key_start:
                        s_past = lax.dot_general(q, k_scr[r, key_start:q_at, cols], nt, preferred_element_type=jnp.float32)
                        m = jnp.maximum(m, jnp.max(s_past, axis=1, keepdims=True))
                    p_diag = jnp.exp((s_diag - m) * scale)
                    total = jnp.sum(p_diag, axis=1, keepdims=True)
                    acc = jnp.dot(p_diag.astype(jnp.bfloat16), v_scr[r, q_at:q_at + piece, cols], preferred_element_type=jnp.float32)
                    if q_at > key_start:
                        p_past = jnp.exp((s_past - m) * scale)
                        total = total + jnp.sum(p_past, axis=1, keepdims=True)
                        acc = acc + jnp.dot(p_past.astype(jnp.bfloat16), v_scr[r, key_start:q_at, cols], preferred_element_type=jnp.float32)
                    slot = q_at // piece - att_base
                    col = pl.multiple_of(step * GROUP + h * HEAD_DIM, HEAD_DIM)
                    att[slot, r * piece:(r + 1) * piece, pl.ds(col, HEAD_DIM)] = (acc / total).astype(jnp.bfloat16)
                    m_top = jnp.max(m)
                    best = m_top if best is None else jnp.maximum(best, m_top)
            top[0, h, :] = jnp.full((top.shape[2],), best * scale, jnp.float32)

    def project_out(slot, o_ref):
        width = wo_scr.shape[1]
        cut = min(512, width)
        for n in range(0, width, cut):
            o = jnp.dot(att[slot], wo_scr[:, n:n + cut], preferred_element_type=jnp.float32).astype(jnp.bfloat16)
            o_ref[:, :, n:n + cut] = o.reshape(rows, piece, cut)

    top[...] = jnp.full(top.shape, -jnp.inf, jnp.float32)

    def work():
        @pl.when(step == 0)
        def _():
            wo_copy().start()

        project(x_own, core, local_off, 2 * chip + core, True)
        project(x_sib, 1 - core, local_off, 2 * chip + 1 - core, True)
        if whole:
            project(x_str, core, remote_off, 2 * (1 - chip) + core, True)
            project(x_crs, 1 - core, remote_off, 2 * (1 - chip) + 1 - core, True)
            attend([j * piece for j in range(4)], 0, 0)
        else:
            @pl.when(chip == 1)
            def _():
                project(x_str, core, remote_off, core, False)
                project(x_crs, 1 - core, remote_off, 1 - core, False)
                attend([2 * piece, 3 * piece], 0, 2)

            @pl.when(chip == 0)
            def _():
                attend([2 * piece, 3 * piece], 2 * piece, 2)

        @pl.when(step == n_steps - 1)
        def _():
            wo_copy().wait()
            project_out(core, o_keep)
            project_out(1 - core, o_send)
            if whole:
                project_out(2 + core, o_str)
                project_out(3 - core, o_crs)

    if whole:
        pl.when(chip == 0)(work)
    else:
        work()


def rows_call(whole, block, out, meta, hidden, sib, straight, cross, w_q, w_k, w_v, w_o, cos_t, sin_t):
    rows, piece, d_model = STEP_ROWS, hidden.shape[1], hidden.shape[2]
    width = w_q.shape[1]
    n_steps = width // GROUP
    n_blocks = hidden.shape[0] // rows
    once = pl.Buffered(1)
    x_block = (rows, piece, d_model)
    x_spec = pl.BlockSpec(x_block, lambda g, m: (0, 0, 0), pipeline_mode=once)
    own_spec = pl.BlockSpec(x_block, lambda g, m: (m[1] * (n_blocks // 2) + block, 0, 0), pipeline_mode=once)
    w_spec = pl.BlockSpec((d_model, GROUP), lambda g, m: (0, g))
    t_spec = pl.BlockSpec(cos_t.shape, lambda g, m: (0, 0), pipeline_mode=once)
    n_out = 4 if whole else 2
    out_shape = [jax.ShapeDtypeStruct(x_block, jnp.bfloat16)] * n_out + [jax.ShapeDtypeStruct((n_steps, 8, 128), jnp.float32)]
    out_specs = [x_spec] * n_out + [pl.BlockSpec((1, 8, 128), lambda g, m: (g, 0, 0))]
    if not whole:
        out_shape[0] = jax.ShapeDtypeStruct(hidden.shape, jnp.bfloat16)
        out_specs[0] = own_spec
    any_spec = pl.BlockSpec(memory_space=pl.ANY)
    chained = out is not None
    tokens = rows * 4 * piece
    flops = tokens * d_model * width * (8 if whole else 6) + 4 * rows * width * 10 * piece * piece
    return pl.pallas_call(
        functools.partial(rows_kernel, whole, chained, piece),
        out_shape=out_shape,
        grid_spec=pltpu.PrefetchScalarGridSpec(
            num_scalar_prefetch=1,
            grid=(n_steps,),
            in_specs=[own_spec, x_spec, x_spec, x_spec, w_spec, w_spec, w_spec, any_spec, t_spec, t_spec] + [any_spec] * chained,
            out_specs=out_specs,
            scratch_shapes=[
                pltpu.VMEM((rows, 4 * piece, GROUP), jnp.bfloat16),
                pltpu.VMEM((rows, 4 * piece, GROUP), jnp.bfloat16),
                pltpu.VMEM((rows, 4 * piece, GROUP), jnp.bfloat16),
                pltpu.VMEM((n_out, rows * piece, width), jnp.bfloat16),
                pltpu.VMEM((width, d_model), jnp.bfloat16),
                pltpu.SemaphoreType.DMA,
            ],
        ),
        compiler_params=pltpu.CompilerParams(dimension_semantics=("arbitrary",), vmem_limit_bytes=66_000_000),
        cost_estimate=pl.CostEstimate(flops=flops, bytes_accessed=60_000_000, transcendentals=0),
        input_output_aliases={11: 0} if chained else {},
        name="whole_rows" if whole else "half_rows",
    )(meta, hidden, sib, straight, cross, w_q, w_k, w_v, w_o, cos_t, sin_t, *([out] if chained else []))


def clip_weights(head_max, w_q, w_k):
    factor = jnp.where(head_max > TAU_CLIP, jnp.sqrt(TAU_CLIP / head_max), 1.0)
    col_factor = jnp.repeat(factor, HEAD_DIM)[None, :]
    return (w_q.astype(jnp.float32) * col_factor).astype(jnp.bfloat16), (w_k.astype(jnp.float32) * col_factor).astype(jnp.bfloat16)


def solution(mesh):
    in_chip = [(0, 1), (1, 0), (2, 3), (3, 2)]
    up_straight, up_cross = [(0, 2), (1, 3)], [(0, 3), (1, 2)]
    down_straight, down_cross = [(2, 0), (3, 1)], [(2, 1), (3, 0)]

    def layer(hidden, pos_ids, w_q, w_k, w_v, w_o):
        rank = lax.axis_index("cp")
        chip, core = rank // 2, rank % 2
        meta = jnp.stack([chip, core]).astype(jnp.int32)
        batch_n = hidden.shape[0]
        half = batch_n // 2
        n_calls = half // STEP_ROWS

        def rows_of(array, which, block):
            return lax.dynamic_slice_in_dim(array, which * half + block * STEP_ROWS, STEP_ROWS, axis=0)

        def send(x, pairs):
            return lax.ppermute(x, "cp", pairs)

        last = n_calls - 1
        order = list(range(n_calls))
        mine, other = [rows_of(hidden, core, 0)], [rows_of(hidden, 1 - core, 0)]
        later, mine[0], other[0] = lax.optimization_barrier((hidden, mine[0], other[0]))
        mine += [rows_of(later, core, b) for b in order[1:]]
        other += [rows_of(later, 1 - core, b) for b in order[1:]]
        straight = [send(mine[b], down_straight if b == last else up_straight) for b in order]
        cross = [send(other[b], down_cross if b == last else up_cross) for b in order]
        sib = [send(other[b], in_chip) for b in order]
        cos_t, sin_t = rope_tables(lax.all_gather(pos_ids, "cp", tiled=True))

        def call(b, out):
            return rows_call(b == last, b, out, meta, hidden, sib[b], straight[b], cross[b], w_q, w_k, w_v, w_o, cos_t, sin_t)

        keep, give, ret_straight, ret_cross, top = call(last, None)
        tops = [top]
        give = send(give, in_chip)
        keep = jnp.where(chip == 1, send(ret_straight, up_straight), keep)
        give = jnp.where(chip == 1, send(ret_cross, up_cross), give)
        out, swapped = None, []
        for b in order[:last]:
            out, swap, top = call(b, out)
            tops.append(top)
            swapped.append(send(swap, in_chip))
        tops = [top[:, :2, 0].reshape(-1) for top in tops]
        for b in order:
            where = (1 - core) * half + b * STEP_ROWS
            out = lax.dynamic_update_slice_in_dim(out, give if b == last else swapped[b], where, axis=0)
        out = lax.dynamic_update_slice_in_dim(out, keep, core * half + last * STEP_ROWS, axis=0)
        head_max = functools.reduce(jnp.maximum, tops)
        head_max = lax.pmax(head_max, ("dp", "cp"))
        w_q_new, w_k_new = clip_weights(head_max, w_q, w_k)
        return out, head_max, w_q_new, w_k_new

    return jax.shard_map(
        layer,
        mesh=mesh,
        in_specs=(P("dp", "cp", None), P("cp"), P(None, None), P(None, None), P(None, None), P(None, None)),
        out_specs=(P("dp", "cp", None), P(None), P(None, None), P(None, None)),
        check_vma=False,
    )
```

```python
import functools

import jax
import jax.numpy as jnp
from jax import lax
from jax.experimental import pallas as pl
from jax.experimental.pallas import tpu as pltpu
from jax.sharding import PartitionSpec as P


HEAD_DIM = 128
TAU_CLIP = 100.0
ROPE_THETA = 50000.0
GROUP = 2 * HEAD_DIM
MOVED_ROWS = 2
NEG = -1e30


def rope_tables(pos_ids):
    half_dim = HEAD_DIM // 2
    inv_freq = jnp.float32(ROPE_THETA) ** (-jnp.arange(half_dim, dtype=jnp.float32) * (2.0 / HEAD_DIM))
    angle = pos_ids.astype(jnp.float32)[:, None] * inv_freq[None, :]
    cos_t, sin_t = jnp.cos(angle), jnp.sin(angle)
    return jnp.concatenate([cos_t, cos_t], axis=-1), jnp.concatenate([-sin_t, sin_t], axis=-1)


def rows_kernel(mode, first_row, meta, hidden, sib, *refs):
    remote = () if mode == "near" else refs[:2]
    w_q, w_k, w_v, w_o, cos_t, sin_t = refs[len(remote):len(remote) + 6]
    n_dst = 4 if mode == "whole" else 2
    out_refs = refs[len(refs) - 5 - n_dst - 1:len(refs) - 5]
    dsts, top = out_refs[:n_dst], out_refs[n_dst]
    x_scr, att, o_scr, wo_scr, sems = refs[len(refs) - 5:]
    row, step = pl.program_id(0), pl.program_id(1)
    n_rows, n_steps = pl.num_programs(0), pl.num_programs(1)
    chip, core = meta[0], meta[1]
    piece = hidden.shape[1]
    half = hidden.shape[0] // 2
    scale = HEAD_DIM ** -0.5
    active = 1 if mode == "far" else 0
    local_at, remote_at = (2, 0) if mode == "far" else (0, 2)

    def load(r, go):
        buf = r % 2

        def one(src, slot, sem):
            at = pl.multiple_of(slot * piece, piece)
            cp = pltpu.make_async_copy(src, x_scr.at[buf, pl.ds(at, piece)], sems.at[buf, sem])
            cp.start() if go else cp.wait()

        one(hidden.at[core * half + first_row + r], local_at + core, 0)
        one(sib.at[first_row + r], local_at + 1 - core, 1)
        if remote:
            one(remote[0].at[r], remote_at + core, 2)
            one(remote[1].at[r], remote_at + 1 - core, 3)

    def store(r, go):
        slots = (core, 1 - core, 2 + core, 3 - core)[:n_dst]
        for n, (dst, slot) in enumerate(zip(dsts, slots)):
            at = pl.multiple_of(slot * piece, piece)
            if mode == "whole":
                to = dst.at[r]
            else:
                to = dst.at[core * half + first_row + r] if n == 0 else dst.at[first_row + r]
            cp = pltpu.make_async_copy(o_scr.at[pl.ds(at, piece)], to, sems.at[2, n])
            cp.start() if go else cp.wait()

    def wo_copy():
        return pltpu.make_async_copy(w_o, wo_scr, sems.at[3, 0])

    def dot(a, b):
        return jnp.dot(a, b, preferred_element_type=jnp.float32)

    def rotated(t, base):
        pos = pl.ds(pl.multiple_of(base * piece, piece), t.shape[0])
        cos_p, sin_p = cos_t[pos, :], sin_t[pos, :]
        parts = []
        for h in range(2):
            th = t[:, h * HEAD_DIM:(h + 1) * HEAD_DIM]
            parts.append((th * cos_p + pltpu.roll(th, HEAD_DIM // 2, axis=1) * sin_p).astype(jnp.bfloat16))
        return parts

    def group():
        buf = row % 2
        x_q_at = 2 * piece if mode == "far" else 0
        n_q = 4 if mode == "whole" else 2
        x_q = x_scr[buf, x_q_at:x_q_at + n_q * piece, :]
        q_base = 2 if mode == "far" else 0
        q = rotated(dot(x_q, w_q[...]), q_base)
        k_own = rotated(dot(x_q, w_k[...]), q_base)
        if mode == "far":
            x_far = x_scr[buf, :2 * piece, :]
            k_far = rotated(dot(x_far, w_k[...]), 0)
        causal = lax.broadcasted_iota(jnp.int32, (piece, piece), 0) >= lax.broadcasted_iota(jnp.int32, (piece, piece), 1)
        nt = (((1,), (1,)), ((), ()))

        def logits(a, b):
            return lax.dot_general(a, b, nt, preferred_element_type=jnp.float32)

        scores = []
        for h in range(2):
            groups = []
            if mode == "far":
                groups.append((0, logits(q[h], k_far[h])))
            for j in range(n_q):
                groups.append((j, logits(q[h][j * piece:], k_own[h][j * piece:(j + 1) * piece])))
            scores.append(groups)
        v_own = dot(x_q, w_v[...]).astype(jnp.bfloat16)
        if mode == "far":
            v_far = dot(x_far, w_v[...]).astype(jnp.bfloat16)
        for h in range(2):
            cols = slice(h * HEAD_DIM, (h + 1) * HEAD_DIM)
            values = [v_far[:, cols]] if mode == "far" else []
            values += [v_own[j * piece:(j + 1) * piece, cols] for j in range(n_q)]
            probs = [[] for _ in values]
            inverse, best = [], None
            for i in range(n_q):
                parts = []
                for g, (start, s) in enumerate(scores[h]):
                    if start <= i:
                        part = s[(i - start) * piece:(i - start + 1) * piece]
                        diagonal = g == len(scores[h]) - n_q + i
                        parts.append((g, jnp.where(causal, part, NEG) if diagonal else part))
                m = functools.reduce(jnp.maximum, [jnp.max(part, axis=1, keepdims=True) for _, part in parts])
                total = None
                for g, part in parts:
                    p = jnp.exp((part - m) * scale)
                    add = jnp.sum(p, axis=1, keepdims=True)
                    total = add if total is None else total + add
                    probs[g].append(p.astype(jnp.bfloat16))
                inverse.append(1.0 / total)
                m_top = jnp.max(m)
                best = m_top if best is None else jnp.maximum(best, m_top)
            weighted = [dot(jnp.concatenate(p, axis=0), v) for p, v in zip(probs, values)]
            col = pl.ds(pl.multiple_of(step * GROUP + h * HEAD_DIM, HEAD_DIM), HEAD_DIM)
            for i in range(n_q):
                acc = None
                for (start, _), w in zip(scores[h], weighted):
                    if start <= i:
                        part = w[(i - start) * piece:(i - start + 1) * piece]
                        acc = part if acc is None else acc + part
                att[i * piece:(i + 1) * piece, col] = (acc * inverse[i]).astype(jnp.bfloat16)
            top[0, 0, h, :] = jnp.full((top.shape[3],), best * scale, jnp.float32)

    top[...] = jnp.full(top.shape, -jnp.inf, jnp.float32)

    @pl.when(chip == active)
    def _():
        @pl.when(step == 0)
        def _():
            @pl.when(row == 0)
            def _():
                load(0, True)
                wo_copy().start()

            load(row, False)

            @pl.when(row + 1 < n_rows)
            def _():
                load(row + 1, True)

        group()

        @pl.when(step == n_steps - 1)
        def _():
            @pl.when(row == 0)
            def _():
                wo_copy().wait()

            width = wo_scr.shape[1]
            cut = min(512, width)
            for n in range(0, width, cut):
                o_scr[:, n:n + cut] = dot(att[...], wo_scr[:, n:n + cut]).astype(jnp.bfloat16)
            store(row, True)
            store(row, False)


def rows_call(mode, first_row, n_rows, chain, meta, hidden, sib, remote, weights, tables):
    piece, d_model = hidden.shape[1:]
    w_q, w_k, w_v, w_o = weights
    width = w_q.shape[1]
    n_steps = width // GROUP
    active = 1 if mode == "far" else 0
    any_spec = pl.BlockSpec(memory_space=pl.ANY)
    w_spec = pl.BlockSpec((d_model, GROUP), lambda r, g, m: (0, jnp.where(m[0] == active, g, 0)))
    t_spec = pl.BlockSpec(tables[0].shape, lambda r, g, m: (0, 0), pipeline_mode=pl.Buffered(1))
    n_q = 4 if mode == "whole" else 2
    x_len = (2 if mode == "near" else 4) * piece
    if mode == "whole":
        out_shape = [jax.ShapeDtypeStruct((n_rows, piece, d_model), jnp.bfloat16)] * 4
    else:
        out_shape = [jax.ShapeDtypeStruct(hidden.shape, jnp.bfloat16), jax.ShapeDtypeStruct(sib.shape, jnp.bfloat16)]
    n_dst = len(out_shape)
    out_shape = out_shape + [jax.ShapeDtypeStruct((n_rows, n_steps, 8, 128), jnp.float32)]
    n_in = 2 + len(remote) + 6
    blocks = {"near": 3, "far": 7, "whole": 10}[mode]
    projections = {"near": 2 * 4, "far": 2 * 6, "whole": 4 * 4}[mode]
    flops = n_rows * (2 * projections * piece * d_model * width + 8 * blocks * piece * piece * width)
    return pl.pallas_call(
        functools.partial(rows_kernel, mode, first_row),
        out_shape=out_shape,
        grid_spec=pltpu.PrefetchScalarGridSpec(
            num_scalar_prefetch=1,
            grid=(n_rows, n_steps),
            in_specs=[any_spec] * (2 + len(remote)) + [w_spec] * 3 + [any_spec, t_spec, t_spec] + [any_spec] * len(chain),
            out_specs=[any_spec] * n_dst + [pl.BlockSpec((1, 1, 8, 128), lambda r, g, m: (r, g, 0, 0))],
            scratch_shapes=[
                pltpu.VMEM((2, x_len, d_model), jnp.bfloat16),
                pltpu.VMEM((n_q * piece, width), jnp.bfloat16),
                pltpu.VMEM((n_q * piece, d_model), jnp.bfloat16),
                pltpu.VMEM((width, d_model), jnp.bfloat16),
                pltpu.SemaphoreType.DMA((4, 4)),
            ],
        ),
        compiler_params=pltpu.CompilerParams(dimension_semantics=("arbitrary", "arbitrary"), vmem_limit_bytes=66_000_000),
        cost_estimate=pl.CostEstimate(flops=flops, bytes_accessed=40_000_000 * n_rows, transcendentals=0),
        input_output_aliases={1 + n_in + n: n for n in range(len(chain))},
    )(meta, hidden, sib, *remote, w_q, w_k, w_v, w_o, *tables, *chain)


def clip_weights(head_max, w_q, w_k):
    factor = jnp.where(head_max > TAU_CLIP, jnp.sqrt(TAU_CLIP / head_max), 1.0)
    col_factor = jnp.repeat(factor, HEAD_DIM)[None, :]
    return (w_q.astype(jnp.float32) * col_factor).astype(jnp.bfloat16), (w_k.astype(jnp.float32) * col_factor).astype(jnp.bfloat16)


def solution(mesh):
    in_chip = [(0, 1), (1, 0), (2, 3), (3, 2)]
    up = [(0, 2), (1, 3)], [(0, 3), (1, 2)]
    down = [(2, 0), (3, 1)], [(2, 1), (3, 0)]

    def layer(hidden, pos_ids, w_q, w_k, w_v, w_o):
        rank = lax.axis_index("cp")
        chip, core = rank // 2, rank % 2
        meta = jnp.stack([chip, core]).astype(jnp.int32)
        half = hidden.shape[0] // 2
        kept = half - MOVED_ROWS
        weights = (w_q, w_k, w_v, w_o)

        def send(x, pairs):
            return lax.ppermute(x, "cp", pairs)

        all_pos, hidden = lax.optimization_barrier((lax.all_gather(pos_ids, "cp", tiled=True), hidden))
        tables = rope_tables(all_pos)

        def row_of(array, which, row):
            return lax.dynamic_slice_in_dim(array, which * half + row, 1, axis=0)

        mine, other = {}, {}
        later = hidden
        for rows in ([0], [kept], [r for r in range(half) if r not in (0, kept)]):
            fetched = [row_of(later, which, r) for r in rows for which in (core, 1 - core)]
            later, *fetched = lax.optimization_barrier((later, *fetched))
            for n, r in enumerate(rows):
                mine[r], other[r] = fetched[2 * n], fetched[2 * n + 1]
        sib = send(lax.dynamic_slice_in_dim(later, (1 - core) * half, half, axis=0), in_chip)
        remote = []
        for r in range(half):
            straight, cross = up if r < kept else down
            remote.append((send(mine[r], straight), send(other[r], cross)))

        def call(mode, row, n_rows, chain):
            far_in = () if mode == "near" else remote[row]
            return rows_call(mode, row, n_rows, chain, meta, hidden, sib, far_in, weights, tables)

        first = (kept + 2) // 3
        out, give, *tops = call("near", 0, first, ())
        wholes = [call("whole", r, 1, ()) for r in range(kept, half)]
        for r in range(kept):
            if r == 2:
                out, give, top = call("near", first, kept - first, (out, give))
                tops.append(top)
            out, give, top = call("far", r, 1, (out, give))
            tops.append(top)
        got = send(give, in_chip)
        out = lax.dynamic_update_slice_in_dim(out, lax.slice_in_dim(got, 0, kept, axis=0), (1 - core) * half, axis=0)
        for r, (keep, pass_on, straight, cross, top) in zip(range(kept, half), wholes):
            tops.append(top)
            pass_on = send(pass_on, in_chip)
            keep = jnp.where(chip == 1, send(straight, up[0]), keep)
            pass_on = jnp.where(chip == 1, send(cross, up[1]), pass_on)
            out = lax.dynamic_update_slice_in_dim(out, keep, core * half + r, axis=0)
            out = lax.dynamic_update_slice_in_dim(out, pass_on, (1 - core) * half + r, axis=0)
        tops = jnp.concatenate([top.max(axis=0)[None, :, :2, 0] for top in tops], axis=0)
        head_max = lax.pmax(lax.pmax(tops.max(axis=0).reshape(-1), "cp"), "dp")
        w_q_new, w_k_new = clip_weights(head_max, w_q, w_k)
        return out, head_max, w_q_new, w_k_new


    return jax.shard_map(
        layer,
        mesh=mesh,
        in_specs=(P("dp", "cp", None), P("cp"), P(None, None), P(None, None), P(None, None), P(None, None)),
        out_specs=(P("dp", "cp", None), P(None), P(None, None), P(None, None)),
        check_vma=False,
    )
```

```python
import functools

import jax
import jax.numpy as jnp
from jax import lax
from jax.experimental import pallas as pl
from jax.experimental.pallas import tpu as pltpu
from jax.sharding import PartitionSpec as P


HEAD_DIM = 128
TAU_CLIP = 100.0
ROPE_THETA = 50000.0
GROUP = 2 * HEAD_DIM
MOVED_ROWS = 2
NEG = -1e30
PACK = {"near": 2, "far": 1, "whole": 1}
CHUNK = 32


def rope_tables(pos_ids):
    half_dim = HEAD_DIM // 2
    inv_freq = jnp.float32(ROPE_THETA) ** (-jnp.arange(half_dim, dtype=jnp.float32) * (2.0 / HEAD_DIM))
    angle = pos_ids.astype(jnp.float32)[:, None] * inv_freq[None, :]
    cos_t, sin_t = jnp.cos(angle), jnp.sin(angle)
    return jnp.concatenate([cos_t, cos_t], axis=-1), jnp.concatenate([-sin_t, sin_t], axis=-1)


def rows_kernel(mode, first_row, meta, hidden, sib, *refs):
    remote = () if mode == "near" else refs[:2]
    w_q, w_k, w_v, w_o, cos_t, sin_t = refs[len(remote):len(remote) + 6]
    n_dst = 4 if mode == "whole" else 2
    out_refs = refs[len(refs) - 5 - n_dst - 1:len(refs) - 5]
    dsts, top = out_refs[:n_dst], out_refs[n_dst]
    x_scr, att, o_scr, wo_scr, sems = refs[len(refs) - 5:]
    row, step = pl.program_id(0), pl.program_id(1)
    n_rows, n_steps = pl.num_programs(0), pl.num_programs(1)
    chip, core = meta[0], meta[1]
    piece = hidden.shape[1]
    half = hidden.shape[0] // 2
    scale = HEAD_DIM ** -0.5
    active = 1 if mode == "far" else 0
    pack = PACK[mode]
    n_q = 4 if mode == "whole" else 2
    span = n_q * piece
    local_at, remote_at = (2, 0) if mode == "far" else (0, 2)

    def load(r, go):
        buf = r % 2

        def one(src, slot, sem):
            at = pl.multiple_of(slot * piece, piece)
            cp = pltpu.make_async_copy(src, x_scr.at[buf, pl.ds(at, piece)], sems.at[buf, sem])
            cp.start() if go else cp.wait()

        for b in range(pack):
            n = first_row + r * pack + b
            one(hidden.at[core * half + n], local_at + core + 2 * b, 2 * b)
            one(sib.at[n], local_at + 1 - core + 2 * b, 2 * b + 1)
        if remote:
            one(remote[0].at[r], remote_at + core, 2)
            one(remote[1].at[r], remote_at + 1 - core, 3)

    def store(r, go):
        slots = (core, 1 - core, 2 + core, 3 - core)[:n_dst]
        for b in range(pack):
            for n, (dst, slot) in enumerate(zip(dsts, slots)):
                at = pl.multiple_of(slot * piece + b * span, piece)
                if mode == "whole":
                    to = dst.at[r]
                else:
                    at_row = first_row + r * pack + b
                    to = dst.at[core * half + at_row] if n == 0 else dst.at[at_row]
                cp = pltpu.make_async_copy(o_scr.at[pl.ds(at, piece)], to, sems.at[2, 2 * b + n])
                cp.start() if go else cp.wait()

    def wo_copy():
        return pltpu.make_async_copy(w_o, wo_scr, sems.at[3, 0])

    def dot(a, b):
        return jnp.dot(a, b, preferred_element_type=jnp.float32)

    def rotated(t, base):
        start = pl.multiple_of(base * piece, piece)
        parts = [[], []]
        for at in range(0, t.shape[0], CHUNK):
            pos = pl.ds(start + at % (n_q * piece), CHUNK)
            cos_p, sin_p = cos_t[pos, :], sin_t[pos, :]
            for h in range(2):
                th = t[at:at + CHUNK, h * HEAD_DIM:(h + 1) * HEAD_DIM]
                parts[h].append((th * cos_p + pltpu.roll(th, HEAD_DIM // 2, axis=1) * sin_p).astype(jnp.bfloat16))
        return [jnp.concatenate(p, axis=0) for p in parts]

    def group():
        buf = row % 2
        x_q_at = 2 * piece if mode == "far" else 0
        x_q = x_scr[buf, x_q_at:x_q_at + pack * span, :]
        q_base = 2 if mode == "far" else 0
        q = rotated(dot(x_q, w_q[...]), q_base)
        k_own = rotated(dot(x_q, w_k[...]), q_base)
        if mode == "far":
            x_far = x_scr[buf, :2 * piece, :]
            k_far = rotated(dot(x_far, w_k[...]), 0)
        nt = (((1,), (1,)), ((), ()))

        def logits(a, b):
            return lax.dot_general(a, b, nt, preferred_element_type=jnp.float32)

        units = [(b, h) for b in range(pack) for h in range(2)]
        scores = []
        for b, h in units:
            groups = []
            q_b, k_b = q[h][b * span:(b + 1) * span], k_own[h][b * span:(b + 1) * span]
            if mode == "far":
                groups.append((0, logits(q_b, k_far[h])))
            for j in range(n_q):
                groups.append((j, logits(q_b[j * piece:], k_b[j * piece:(j + 1) * piece])))
            scores.append(groups)
        v_own = dot(x_q, w_v[...]).astype(jnp.bfloat16)
        if mode == "far":
            v_far = dot(x_far, w_v[...]).astype(jnp.bfloat16)
        tops = [None, None]
        rows = lax.broadcasted_iota(jnp.int32, (CHUNK, piece), 0)
        lanes = lax.broadcasted_iota(jnp.int32, (CHUNK, piece), 1)
        for (b, h), groups in zip(units, scores):
            cols = slice(h * HEAD_DIM, (h + 1) * HEAD_DIM)
            values = [v_far[:, cols]] if mode == "far" else []
            values += [v_own[b * span + j * piece:b * span + (j + 1) * piece, cols] for j in range(n_q)]
            probs = [[] for _ in values]
            inverse = []
            for at in range(0, span, CHUNK):
                i = at // piece
                parts = []
                for g, (start, s) in enumerate(groups):
                    if start <= i:
                        part = s[at - start * piece:at - start * piece + CHUNK]
                        diagonal = g == len(groups) - n_q + i
                        parts.append((g, jnp.where(rows + (at - i * piece) >= lanes, part, NEG) if diagonal else part))
                m = functools.reduce(jnp.maximum, [jnp.max(part, axis=1, keepdims=True) for _, part in parts])
                total = None
                for g, part in parts:
                    p = jnp.exp((part - m) * scale)
                    add = jnp.sum(p, axis=1, keepdims=True)
                    total = add if total is None else total + add
                    probs[g].append(p.astype(jnp.bfloat16))
                inverse.append(1.0 / total)
                tops[h] = m if tops[h] is None else jnp.maximum(tops[h], m)
            weighted = [dot(jnp.concatenate(p, axis=0), v) for p, v in zip(probs, values)]
            col = pl.ds(pl.multiple_of(step * GROUP + h * HEAD_DIM, HEAD_DIM), HEAD_DIM)
            for n, at in enumerate(range(0, span, CHUNK)):
                acc = None
                for (start, _), w in zip(groups, weighted):
                    if start * piece <= at:
                        part = w[at - start * piece:at - start * piece + CHUNK]
                        acc = part if acc is None else acc + part
                att[b * span + at:b * span + at + CHUNK, col] = (acc * inverse[n]).astype(jnp.bfloat16)
        for h in range(2):
            top[0, 0, h, :] = jnp.full((top.shape[3],), jnp.max(tops[h]) * scale, jnp.float32)

    top[...] = jnp.full(top.shape, -jnp.inf, jnp.float32)

    @pl.when(chip == active)
    def _():
        @pl.when(step == 0)
        def _():
            @pl.when(row == 0)
            def _():
                load(0, True)
                wo_copy().start()

            load(row, False)

            @pl.when(row + 1 < n_rows)
            def _():
                load(row + 1, True)

        group()

        @pl.when(step == n_steps - 1)
        def _():
            @pl.when(row == 0)
            def _():
                wo_copy().wait()

            width = wo_scr.shape[1]
            cut = min(512, width)
            for n in range(0, width, cut):
                o_scr[:, n:n + cut] = dot(att[...], wo_scr[:, n:n + cut]).astype(jnp.bfloat16)
            store(row, True)
            store(row, False)


def rows_call(mode, first_row, n_rows, chain, meta, hidden, sib, remote, weights, tables):
    piece, d_model = hidden.shape[1:]
    w_q, w_k, w_v, w_o = weights
    width = w_q.shape[1]
    n_steps = width // GROUP
    active = 1 if mode == "far" else 0
    any_spec = pl.BlockSpec(memory_space=pl.ANY)
    w_spec = pl.BlockSpec((d_model, GROUP), lambda r, g, m: (0, jnp.where(m[0] == active, g, 0)))
    t_spec = pl.BlockSpec(tables[0].shape, lambda r, g, m: (0, 0), pipeline_mode=pl.Buffered(1))
    pack = PACK[mode]
    n_q = pack * (4 if mode == "whole" else 2)
    x_len = 4 * piece
    if mode == "whole":
        out_shape = [jax.ShapeDtypeStruct((n_rows, piece, d_model), jnp.bfloat16)] * 4
    else:
        out_shape = [jax.ShapeDtypeStruct(hidden.shape, jnp.bfloat16), jax.ShapeDtypeStruct(sib.shape, jnp.bfloat16)]
    n_dst = len(out_shape)
    out_shape = out_shape + [jax.ShapeDtypeStruct((n_rows // pack, n_steps, 8, 128), jnp.float32)]
    n_in = 2 + len(remote) + 6
    blocks = {"near": 3, "far": 7, "whole": 10}[mode]
    projections = {"near": 2 * 4, "far": 2 * 6, "whole": 4 * 4}[mode]
    flops = n_rows * (2 * projections * piece * d_model * width + 8 * blocks * piece * piece * width)
    *results, top = pl.pallas_call(
        functools.partial(rows_kernel, mode, first_row),
        out_shape=out_shape,
        grid_spec=pltpu.PrefetchScalarGridSpec(
            num_scalar_prefetch=1,
            grid=(n_rows // pack, n_steps),
            in_specs=[any_spec] * (2 + len(remote)) + [w_spec] * 3 + [any_spec, t_spec, t_spec] + [any_spec] * len(chain),
            out_specs=[any_spec] * n_dst + [pl.BlockSpec((1, 1, 8, 128), lambda r, g, m: (r, g, 0, 0))],
            scratch_shapes=[
                pltpu.VMEM((2, x_len, d_model), jnp.bfloat16),
                pltpu.VMEM((n_q * piece, width), jnp.bfloat16),
                pltpu.VMEM((n_q * piece, d_model), jnp.bfloat16),
                pltpu.VMEM((width, d_model), jnp.bfloat16),
                pltpu.SemaphoreType.DMA((4, 4)),
            ],
        ),
        compiler_params=pltpu.CompilerParams(dimension_semantics=("arbitrary", "arbitrary"), vmem_limit_bytes=66_000_000),
        cost_estimate=pl.CostEstimate(flops=flops, bytes_accessed=40_000_000 * n_rows, transcendentals=0),
        input_output_aliases={1 + n_in + n: n for n in range(len(chain))},
    )(meta, hidden, sib, *remote, w_q, w_k, w_v, w_o, *tables, *chain)
    return *results, top.max(axis=0, keepdims=True)


def clip_weights(head_max, w_q, w_k):
    factor = jnp.where(head_max > TAU_CLIP, jnp.sqrt(TAU_CLIP / head_max), 1.0)
    col_factor = jnp.repeat(factor, HEAD_DIM)[None, :]
    return (w_q.astype(jnp.float32) * col_factor).astype(jnp.bfloat16), (w_k.astype(jnp.float32) * col_factor).astype(jnp.bfloat16)


def solution(mesh):
    in_chip = [(0, 1), (1, 0), (2, 3), (3, 2)]
    up = [(0, 2), (1, 3)], [(0, 3), (1, 2)]
    down = [(2, 0), (3, 1)], [(2, 1), (3, 0)]

    def layer(hidden, pos_ids, w_q, w_k, w_v, w_o):
        rank = lax.axis_index("cp")
        chip, core = rank // 2, rank % 2
        meta = jnp.stack([chip, core]).astype(jnp.int32)
        half = hidden.shape[0] // 2
        kept = half - MOVED_ROWS
        weights = (w_q, w_k, w_v, w_o)

        def send(x, pairs):
            return lax.ppermute(x, "cp", pairs)

        all_pos, hidden = lax.optimization_barrier((lax.all_gather(pos_ids, "cp", tiled=True), hidden))
        tables = rope_tables(all_pos)

        def row_of(array, which, row):
            return lax.dynamic_slice_in_dim(array, which * half + row, 1, axis=0)

        mine, other = {}, {}
        sib = lax.dynamic_slice_in_dim(hidden, (1 - core) * half, half, axis=0)
        later, sib = lax.optimization_barrier((hidden, sib))
        sib = send(sib, in_chip)
        early = [0, 1, kept]
        for rows in ([0], early[1:], [r for r in range(half) if r not in early]):
            fetched = [row_of(later, which, r) for r in rows for which in (core, 1 - core)]
            later, *fetched = lax.optimization_barrier((later, *fetched))
            for n, r in enumerate(rows):
                mine[r], other[r] = fetched[2 * n], fetched[2 * n + 1]
        remote = []
        for r in range(half):
            straight, cross = up if r < kept else down
            remote.append((send(mine[r], straight), send(other[r], cross)))

        def call(mode, row, n_rows, chain):
            far_in = () if mode == "near" else remote[row]
            return rows_call(mode, row, n_rows, chain, meta, hidden, sib, far_in, weights, tables)

        first = (kept + 2) // 3
        out, give, *tops = call("near", 0, first, ())
        wholes = [call("whole", r, 1, ()) for r in range(kept, half)]
        for r in range(kept):
            if r == 2:
                out, give, top = call("near", first, kept - first, (out, give))
                tops.append(top)
            out, give, top = call("far", r, 1, (out, give))
            tops.append(top)
        got = send(give, in_chip)
        out = lax.dynamic_update_slice_in_dim(out, lax.slice_in_dim(got, 0, kept, axis=0), (1 - core) * half, axis=0)
        for r, (keep, pass_on, straight, cross, top) in zip(range(kept, half), wholes):
            tops.append(top)
            pass_on = send(pass_on, in_chip)
            keep = jnp.where(chip == 1, send(straight, up[0]), keep)
            pass_on = jnp.where(chip == 1, send(cross, up[1]), pass_on)
            out = lax.dynamic_update_slice_in_dim(out, keep, core * half + r, axis=0)
            out = lax.dynamic_update_slice_in_dim(out, pass_on, (1 - core) * half + r, axis=0)
        head_max = functools.reduce(jnp.maximum, tops)[0, :, :2, 0].reshape(-1)
        head_max = lax.pmax(lax.all_gather(head_max, "cp").max(axis=0), "dp")
        w_q_new, w_k_new = clip_weights(head_max, w_q, w_k)
        return out, head_max, w_q_new, w_k_new


    return jax.shard_map(
        layer,
        mesh=mesh,
        in_specs=(P("dp", "cp", None), P("cp"), P(None, None), P(None, None), P(None, None), P(None, None)),
        out_specs=(P("dp", "cp", None), P(None), P(None, None), P(None, None)),
        check_vma=False,
    )
```
